16 devices in a mesh: dp: 2 (over y, z), tp: 8 (over x, core).
Axes of the slice: x: 4, y: 2, z: 1, core: 2. Of those that a mesh axis runs over, the one named last changes fastest.
The devices are a block of a 4x4x8 slice.
Arguments:
- x: bfloat16 [4096, 2048], P('dp'), parts along dimension 0
- w_gate: bfloat16 [2048, 8192], P(None, 'tp')
- w_up: bfloat16 [2048, 8192], P(None, 'tp')
- w_down: bfloat16 [8192, 2048], P('tp')
Outputs:
- output: bfloat16 [4096, 2048], P('dp'), parts along dimension 0
There are 2 independent parts. The reference program is written for one: setup_inputs(seed, part) draws one part's arguments, and reference() takes and returns one part's arrays. A program takes and returns all parts, laid end to end along the dimension named above; an argument that names none is the same for every part.
All inputs are finite; a program needn't handle non-finite values.
Results may differ from the reference program's by a relative error of at most 0.016.
Values are sent between devices in bfloat16 or wider.
A program may use at most 768 MiB of HBM per device.

```python
import jax
import jax.numpy as jnp

ROWS = 2048
D = 2048
FF = 8192


def setup_inputs(seed: int = 0, part: int = 0) -> dict:
    kx, kg, ku, kd = jax.random.split(jax.random.key(seed), 4)
    drawn = {
        "x": jax.random.normal(jax.random.fold_in(kx, part), (ROWS, D), jnp.float32),
        "w_gate": jax.random.normal(kg, (D, FF), jnp.float32) * D**-0.5,
        "w_up": jax.random.normal(ku, (D, FF), jnp.float32) * D**-0.5,
        "w_down": jax.random.normal(kd, (FF, D), jnp.float32) * FF**-0.5,
    }
    return {k: v.astype(jnp.bfloat16) for k, v in drawn.items()}


def reference(x, w_gate, w_up, w_down):
    gate = jnp.dot(x, w_gate, preferred_element_type=jnp.float32)
    up = jnp.dot(x, w_up, preferred_element_type=jnp.float32)
    hidden = (jax.nn.silu(gate) * up).astype(jnp.bfloat16)
    return jnp.dot(hidden, w_down, preferred_element_type=jnp.float32).astype(jnp.bfloat16)
```

```python
import functools

import jax
import jax.numpy as jnp
from jax import lax
from jax.experimental import pallas as pl
from jax.experimental.pallas import tpu as pltpu
from jax.sharding import PartitionSpec as P

MESH = pl.DeviceIdType.MESH
F32, BF16 = jnp.float32, jnp.bfloat16
CORES = 2
SUBS = 2
FIRST_TILES, GATE_TILES = 4, 2
FIRST_CUTS, CUTS = 4, 2
LAST_CUTS = 4
GROUP = 16


def tile(i, width):
    start = i * width
    return pl.ds(start if isinstance(start, int) else pl.multiple_of(start, width), width)


def mlp_kernel(n, x, wg, wu, wd, y, xs, wgv, wuv, wdv, hid, own, give, got, part, run, *sems):
    (x_sem, g_sem, u_sem, d_sem, give_sem, got_sem, part_sem, run_sem, gs_sem, gr_sem, os_sem, or_sem) = sems
    rows, depth = x.shape
    units = wg.shape[1]
    chunk = rows // n
    half = chunk // CORES
    p = half // SUBS
    blocks = n * SUBS

    me = lax.axis_index("tp")
    chip, core = me // CORES, me % CORES
    way = 1 - 2 * core
    peer = me + way
    ahead = ((chip + way + n) % n) * CORES + core
    behind = ((chip - way + n) % n) * CORES + core

    def my_rows(s, j):
        start = ((chip - way * (1 + s) + n) % n) * chunk + core * half + j * p
        return pl.multiple_of(start, p)

    def peer_rows(s, j):
        start = ((chip + way * (1 + s) + n) % n) * chunk + (1 - core) * half + j * p
        return pl.multiple_of(start, p)

    def remote(src, dst, ssem, rsem, to):
        return pltpu.make_async_remote_copy(
            src_ref=src, dst_ref=dst, send_sem=ssem, recv_sem=rsem, device_id={"tp": to}, device_id_type=MESH
        )

    barrier = pltpu.get_barrier_semaphore()
    for other in (peer, ahead, behind):
        pl.semaphore_signal(barrier, inc=1, device_id={"tp": other}, device_id_type=MESH)

    def x_copies(b):
        s, j = b // SUBS, b % SUBS
        return (
            pltpu.make_async_copy(x.at[pl.ds(my_rows(s, j), p)], xs.at[b, pl.ds(0, p)], x_sem.at[b, 0]),
            pltpu.make_async_copy(x.at[pl.ds(peer_rows(s, j), p)], xs.at[b, pl.ds(p, p)], x_sem.at[b, 1]),
        )

    def gate_copies(i):
        c = tile(i, units // FIRST_TILES)
        return (
            pltpu.make_async_copy(wg.at[:, c], wgv.at[:, c], g_sem.at[i]),
            pltpu.make_async_copy(wu.at[:, c], wuv.at[:, c], u_sem.at[i]),
        )

    def down_copy(i):
        c = tile(i, depth // FIRST_CUTS)
        return pltpu.make_async_copy(wd.at[:, c], wdv.at[:, c], d_sem.at[i])

    for c in x_copies(0):
        c.start()
    for i in range(FIRST_TILES):
        for c in gate_copies(i):
            c.start()
    for i in range(FIRST_CUTS):
        down_copy(i).start()

    def hidden(b, i, tiles):
        c = tile(i, units // tiles)
        g = jnp.dot(xs[b], wgv[:, c], preferred_element_type=F32)
        u = jnp.dot(xs[b], wuv[:, c], preferred_element_type=F32)
        hid[:, c] = (jax.nn.silu(g) * u).astype(BF16)

    def give_copy(b, q, cuts):
        c = tile(q, depth // cuts)
        return remote(give.at[b, :, c], got.at[b, :, c], give_sem.at[b, q], got_sem.at[b, q], peer)

    def down(b, q, cuts):
        c = tile(q, depth // cuts)
        term = jnp.dot(hid[...], wdv[:, c], preferred_element_type=F32)
        own[b, :, c] = term[:p]
        give[b, :, c] = term[p:].astype(BF16)
        give_copy(b, q, cuts).start()

    def run_copy(b, q, cuts):
        c = tile(q, depth // cuts)
        return remote(part.at[b, :, c], run.at[b, :, c], part_sem.at[b, q], run_sem.at[b, q], ahead)

    def ring_copy(k, j, q, cuts):
        at = pl.ds(my_rows(k - 1, j) + q * (p // cuts), p // cuts)
        return remote(y.at[at], y.at[at], gs_sem.at[k * SUBS + j, q], gr_sem.at[k * SUBS + j, q], ahead)

    def over_copy(k, j, q, cuts):
        at = pl.ds(my_rows(k - 1, j) + q * (p // cuts), p // cuts)
        return remote(y.at[at], y.at[at], os_sem.at[k * SUBS + j, q], or_sem.at[k * SUBS + j, q], peer)

    def over_arrival(k, j, q, cuts):
        at = pl.ds(peer_rows(k - 1, j) + q * (p // cuts), p // cuts)
        return remote(y.at[at], y.at[at], os_sem.at[k * SUBS + j, q], or_sem.at[k * SUBS + j, q], peer)

    def ring_arrival(k, j, q, cuts):
        at = pl.ds(my_rows(k, j) + q * (p // cuts), p // cuts)
        return remote(y.at[at], y.at[at], gs_sem.at[k * SUBS + j, q], gr_sem.at[k * SUBS + j, q], ahead)

    def cuts_of(b):
        return FIRST_CUTS if b == 0 else CUTS

    def hop_cuts(k):
        return LAST_CUTS if k == n - 2 else 1

    def over_cuts(k):
        return LAST_CUTS if k == n - 1 else 1

    def add(b, c, before, dst, base):
        def body(i, _):
            at = tile(i, GROUP)
            total = own[b, at, c] + got[b, at, c].astype(F32)
            if before:
                total = total + run[b - SUBS, at, c].astype(F32)
            if dst is y:
                y[pl.ds(pl.multiple_of(base + i * GROUP, GROUP), GROUP), c] = total.astype(BF16)
            else:
                part[b, at, c] = total.astype(BF16)
            return 0

        lax.fori_loop(0, p // GROUP, body, 0)

    for b in range(blocks):
        s, j = b // SUBS, b % SUBS
        tiles, cuts = (FIRST_TILES if b == 0 else GATE_TILES), cuts_of(b)
        for c in x_copies(b):
            c.wait()

        def gate_up(i, _):
            if b == 0:
                for c in gate_copies(i):
                    c.wait()
            hidden(b, i, tiles)
            return 0

        lax.fori_loop(0, tiles, gate_up, 0)
        if b == 0:
            for later in range(1, blocks):
                for c in x_copies(later):
                    c.start()
            pl.semaphore_wait(barrier, 3)

        def out(q, _):
            if b == 0:
                down_copy(q).wait()
            down(b, q, cuts)
            return 0

        lax.fori_loop(0, cuts, out, 0)

        if s > 0:
            for q in range(cuts_of(b - SUBS)):
                run_copy(b - SUBS, q, cuts_of(b - SUBS)).wait_recv()
        for q in range(cuts):
            give_copy(b, q, cuts).wait_recv()
            c = tile(q, depth // cuts)
            if s < n - 1:
                add(b, c, s > 0, part, 0)
                run_copy(b, q, cuts).start()
            else:
                add(b, c, True, y, my_rows(s, j))
        if s == n - 1:
            for q in range(hop_cuts(0)):
                ring_copy(0, j, q, hop_cuts(0)).start()
            for q in range(over_cuts(0)):
                over_copy(0, j, q, over_cuts(0)).start()

    for k in range(n - 1):
        for j in range(SUBS):
            cuts = hop_cuts(k)
            for q in range(cuts):
                ring_arrival(k, j, q, cuts).wait_recv()
                if over_cuts(k + 1) == cuts:
                    over_copy(k + 1, j, q, cuts).start()
            if k + 1 < n - 1:
                for q in range(hop_cuts(k + 1)):
                    ring_copy(k + 1, j, q, hop_cuts(k + 1)).start()

    for b in range(blocks):
        for q in range(cuts_of(b)):
            give_copy(b, q, cuts_of(b)).wait_send()
            if b // SUBS < n - 1:
                run_copy(b, q, cuts_of(b)).wait_send()
    for k in range(n):
        for j in range(SUBS):
            if k < n - 1:
                for q in range(hop_cuts(k)):
                    ring_copy(k, j, q, hop_cuts(k)).wait_send()
            for q in range(over_cuts(k)):
                over_copy(k, j, q, over_cuts(k)).wait_send()
                over_arrival(k, j, q, over_cuts(k)).wait_recv()


def write_kernel(pieces, y, out, sem):
    r = y.shape[0] // pieces
    copies = [pltpu.make_async_copy(y.at[tile(i, r)], out.at[tile(i, r)], sem.at[i]) for i in range(pieces)]
    for c in copies:
        c.start()
    for c in copies:
        c.wait()


def solution(mesh):
    n = mesh.shape["tp"] // CORES

    def step(x, w_gate, w_up, w_down):
        rows, depth = x.shape
        units = w_gate.shape[1]
        p = rows // n // CORES // SUBS
        blocks = n * SUBS
        dma = pltpu.SemaphoreType.DMA
        most = max(FIRST_CUTS, CUTS)
        y = pl.pallas_call(
            functools.partial(mlp_kernel, n),
            out_shape=pltpu.VMEM((rows, depth), BF16),
            in_specs=[pl.BlockSpec(memory_space=pl.ANY)] * 4,
            out_specs=pl.BlockSpec(memory_space=pltpu.VMEM),
            scratch_shapes=[
                pltpu.VMEM((blocks, CORES * p, depth), BF16),
                pltpu.VMEM((depth, units), BF16),
                pltpu.VMEM((depth, units), BF16),
                pltpu.VMEM((units, depth), BF16),
                pltpu.VMEM((CORES * p, units), BF16),
                pltpu.VMEM((blocks, p, depth), F32),
                pltpu.VMEM((blocks, p, depth), BF16),
                pltpu.VMEM((blocks, p, depth), BF16),
                pltpu.VMEM((blocks - SUBS, p, depth), BF16),
                pltpu.VMEM((blocks - SUBS, p, depth), BF16),
                dma((blocks, CORES)),
                dma((FIRST_TILES,)),
                dma((FIRST_TILES,)),
                dma((FIRST_CUTS,)),
                dma((blocks, most)),
                dma((blocks, most)),
                dma((blocks - SUBS, most)),
                dma((blocks - SUBS, most)),
                dma((blocks - SUBS, LAST_CUTS)),
                dma((blocks - SUBS, LAST_CUTS)),
                dma((blocks, LAST_CUTS)),
                dma((blocks, LAST_CUTS)),
            ],
            compiler_params=pltpu.CompilerParams(
                collective_id=0, has_side_effects=True, vmem_limit_bytes=52 * 2**20
            ),
            cost_estimate=pl.CostEstimate(
                flops=6 * rows * depth * units, bytes_accessed=2 * rows * depth + 6 * depth * units, transcendentals=rows * units
            ),
        )(x, w_gate, w_up, w_down)
        pieces = 8
        return pl.pallas_call(
            functools.partial(write_kernel, pieces),
            out_shape=jax.ShapeDtypeStruct((rows, depth), BF16),
            in_specs=[pl.BlockSpec(memory_space=pltpu.VMEM)],
            out_specs=pl.BlockSpec(memory_space=pltpu.HBM),
            scratch_shapes=[dma((pieces,))],
            compiler_params=pltpu.CompilerParams(has_side_effects=True, vmem_limit_bytes=4 * 2**20),
        )(y)

    return jax.shard_map(
        step,
        mesh=mesh,
        in_specs=(P("dp", None), P(None, "tp"), P(None, "tp"), P("tp", None)),
        out_specs=P("dp", None),
        check_vma=False,
    )
```

```python
import functools

import jax
import jax.numpy as jnp
from jax import lax
from jax.experimental import pallas as pl
from jax.experimental.pallas import tpu as pltpu
from jax.sharding import PartitionSpec as P

MESH = pl.DeviceIdType.MESH
F32, BF16 = jnp.float32, jnp.bfloat16
CORES = 2
SUBS = 2
FIRST_TILES, GATE_TILES = 4, 2
FIRST_CUTS, CUTS = 4, 2
LAST_CUTS = 4
GROUP = 16


def tile(i, width):
    start = i * width
    return pl.ds(start if isinstance(start, int) else pl.multiple_of(start, width), width)


def mlp_kernel(n, x, wg, wu, wd, y, xs, wgv, wuv, wdv, hid, own, give, got, part, run, *sems):
    x_sem, g_sem, d_sem, give_sem, got_sem, part_sem, run_sem, ring_sem, ringed_sem, over_sem, overed_sem = sems
    rows, depth = x.shape
    units = wg.shape[1]
    chunk = rows // n
    half = chunk // CORES
    p = half // SUBS
    blocks = n * SUBS

    me = lax.axis_index("tp")
    chip, core = me // CORES, me % CORES
    way = 1 - 2 * core
    peer = me + way
    ahead = ((chip + way + n) % n) * CORES + core
    behind = ((chip - way + n) % n) * CORES + core

    def my_rows(s, j):
        start = ((chip - way * (1 + s) + n) % n) * chunk + core * half + j * p
        return pl.multiple_of(start, p)

    def peer_rows(s, j):
        start = ((chip + way * (1 + s) + n) % n) * chunk + (1 - core) * half + j * p
        return pl.multiple_of(start, p)

    def remote(src, dst, ssem, rsem, to):
        return pltpu.make_async_remote_copy(
            src_ref=src, dst_ref=dst, send_sem=ssem, recv_sem=rsem, device_id={"tp": to}, device_id_type=MESH
        )

    barrier = pltpu.get_barrier_semaphore()
    for other in (peer, ahead, behind):
        pl.semaphore_signal(barrier, inc=1, device_id={"tp": other}, device_id_type=MESH)

    def x_copies(b):
        s, j = b // SUBS, b % SUBS
        return (
            pltpu.make_async_copy(x.at[pl.ds(my_rows(s, j), p)], xs.at[b, pl.ds(0, p)], x_sem.at[b]),
            pltpu.make_async_copy(x.at[pl.ds(peer_rows(s, j), p)], xs.at[b, pl.ds(p, p)], x_sem.at[b]),
        )

    def gate_copies(i):
        c = tile(i, units // FIRST_TILES)
        return (
            pltpu.make_async_copy(wg.at[:, c], wgv.at[:, c], g_sem.at[i]),
            pltpu.make_async_copy(wu.at[:, c], wuv.at[:, c], g_sem.at[i]),
        )

    def down_copy(i):
        c = tile(i, depth // FIRST_CUTS)
        return pltpu.make_async_copy(wd.at[:, c], wdv.at[:, c], d_sem.at[i])

    def start(*copies, later=1):
        for c in copies:
            c.start(priority=later)

    start(*x_copies(0), *gate_copies(0), later=0)
    start(*gate_copies(1))

    def hidden(b, i, tiles):
        c = tile(i, units // tiles)
        g = jnp.dot(xs[b], wgv[:, c], preferred_element_type=F32)
        u = jnp.dot(xs[b], wuv[:, c], preferred_element_type=F32)
        hid[:, c] = (jax.nn.silu(g) * u).astype(BF16)

    def got_at(b, q):
        return q if b == 0 else FIRST_CUTS + q if b == 1 else FIRST_CUTS + CUTS + b - 2

    def give_copy(b, q, cuts):
        c = tile(q, depth // cuts)
        return remote(give.at[b, :, c], got.at[b, :, c], give_sem, got_sem.at[got_at(b, q)], peer)

    def gave(b):
        return remote(give.at[b], got.at[b], give_sem, got_sem.at[got_at(b, 0)], peer)

    def down(b, q, cuts):
        c = tile(q, depth // cuts)
        term = jnp.dot(hid[...], wdv[:, c], preferred_element_type=F32)
        own[b, :, c] = term[:p]
        give[b, :, c] = term[p:].astype(BF16)
        give_copy(b, q, cuts).start()

    def run_copy(b, q, cuts):
        c = tile(q, depth // cuts)
        return remote(part.at[b, :, c], run.at[b, :, c], part_sem, run_sem.at[b], ahead)

    def ran(b):
        return remote(part.at[b], run.at[b], part_sem, run_sem.at[b], ahead)

    def ring_copy(k, j, q, cuts):
        at = pl.ds(my_rows(k - 1, j) + q * (p // cuts), p // cuts)
        return remote(y.at[at], y.at[at], ring_sem, ringed_sem.at[k * SUBS + j * cuts + q], ahead)

    def over_copy(k, j, q, cuts):
        at = pl.ds(my_rows(k - 1, j) + q * (p // cuts), p // cuts)
        return remote(y.at[at], y.at[at], over_sem, overed_sem, peer)

    def cuts_of(b):
        return FIRST_CUTS if b == 0 else CUTS

    def hop_cuts(k):
        return LAST_CUTS if k == n - 2 else 1

    def over_cuts(k):
        return LAST_CUTS if k == n - 1 else 1

    def add(b, c, before, dst, base):
        def body(i, _):
            at = tile(i, GROUP)
            total = own[b, at, c] + got[b, at, c].astype(F32)
            if before:
                total = total + run[b - SUBS, at, c].astype(F32)
            if dst is y:
                y[pl.ds(pl.multiple_of(base + i * GROUP, GROUP), GROUP), c] = total.astype(BF16)
            else:
                part[b, at, c] = total.astype(BF16)
            return 0

        lax.fori_loop(0, p // GROUP, body, 0)

    def finish(b, q):
        s, j, cuts = b // SUBS, b % SUBS, cuts_of(b)
        c = tile(q, depth // cuts)
        if s < n - 1:
            add(b, c, s > 0, part, 0)
            run_copy(b, q, cuts).start()
        else:
            add(b, c, True, y, my_rows(s, j))

    for c in x_copies(0):
        c.wait()
    for i in range(FIRST_TILES):
        for c in gate_copies(i):
            c.wait()
        if i + 2 < FIRST_TILES:
            start(*gate_copies(i + 2))
        elif i + 2 == FIRST_TILES:
            start(down_copy(0), down_copy(1))
        else:
            start(*[down_copy(q) for q in range(2, FIRST_CUTS)])
        hidden(0, i, FIRST_TILES)
    pl.semaphore_wait(barrier, 3)
    for q in range(FIRST_CUTS):
        down_copy(q).wait()
        if q == FIRST_CUTS - 1:
            start(*x_copies(1), *x_copies(2))
            give_copy(0, 0, FIRST_CUTS).wait_recv()
            finish(0, 0)
        down(0, q, FIRST_CUTS)
    def arrive(b):
        for c in x_copies(b):
            c.wait()

    for q in range(1, FIRST_CUTS):
        if q == FIRST_CUTS - 1:
            arrive(1)
            hidden(1, 0, GATE_TILES)
        give_copy(0, q, FIRST_CUTS).wait_recv()
        finish(0, q)
    for b in range(3, blocks):
        start(*x_copies(b))

    for b in range(1, blocks):
        s, j = b // SUBS, b % SUBS
        for i in range(1, GATE_TILES):
            hidden(b, i, GATE_TILES)

        def out(q, _):
            down(b, q, CUTS)
            return 0

        lax.fori_loop(0, CUTS, out, 0)
        if b == 1:
            for q in range(CUTS - 1):
                give_copy(b, q, CUTS).wait_recv()
                finish(b, q)
        if b + 1 < blocks:
            arrive(b + 1)
            hidden(b + 1, 0, GATE_TILES)
        if b == 1:
            give_copy(b, CUTS - 1, CUTS).wait_recv()
            finish(b, CUTS - 1)
            continue
        if s > 0:
            ran(b - SUBS).wait_recv()
        gave(b).wait_recv()
        for q in range(CUTS):
            finish(b, q)
        if s == n - 1:
            for q in range(hop_cuts(0)):
                ring_copy(0, j, q, hop_cuts(0)).start()
            for q in range(over_cuts(0)):
                over_copy(0, j, q, over_cuts(0)).start()

    for k in range(n - 1):
        for j in range(SUBS):
            cuts = hop_cuts(k)
            for q in range(cuts):
                ring_copy(k, j, q, cuts).wait_recv()
                if over_cuts(k + 1) == cuts:
                    over_copy(k + 1, j, q, cuts).start()
            if k + 1 < n - 1:
                for q in range(hop_cuts(k + 1)):
                    ring_copy(k + 1, j, q, hop_cuts(k + 1)).start()

    whole = y.at[pl.ds(0, rows // CORES)]
    remote(give, got, give_sem, got_sem.at[0], peer).wait_send()
    remote(part, run, part_sem, run_sem.at[0], ahead).wait_send()
    remote(y.at[pl.ds(0, (n - 1) * half)], y.at[pl.ds(0, (n - 1) * half)], ring_sem, ringed_sem.at[0], ahead).wait_send()
    remote(whole, whole, over_sem, overed_sem, peer).wait()


def write_kernel(pieces, y, out, sem):
    r = y.shape[0] // pieces
    copies = [pltpu.make_async_copy(y.at[tile(i, r)], out.at[tile(i, r)], sem.at[i]) for i in range(pieces)]
    for c in copies:
        c.start()
    for c in copies:
        c.wait()


def solution(mesh):
    n = mesh.shape["tp"] // CORES

    def step(x, w_gate, w_up, w_down):
        rows, depth = x.shape
        units = w_gate.shape[1]
        p = rows // n // CORES // SUBS
        blocks = n * SUBS
        dma = pltpu.SemaphoreType.DMA
        y = pl.pallas_call(
            functools.partial(mlp_kernel, n),
            out_shape=pltpu.VMEM((rows, depth), BF16),
            in_specs=[pl.BlockSpec(memory_space=pl.ANY)] * 4,
            out_specs=pl.BlockSpec(memory_space=pltpu.VMEM),
            scratch_shapes=[
                pltpu.VMEM((blocks, CORES * p, depth), BF16),
                pltpu.VMEM((depth, units), BF16),
                pltpu.VMEM((depth, units), BF16),
                pltpu.VMEM((units, depth), BF16),
                pltpu.VMEM((CORES * p, units), BF16),
                pltpu.VMEM((blocks, p, depth), F32),
                pltpu.VMEM((blocks, p, depth), BF16),
                pltpu.VMEM((blocks, p, depth), BF16),
                pltpu.VMEM((blocks - SUBS, p, depth), BF16),
                pltpu.VMEM((blocks - SUBS, p, depth), BF16),
                dma((blocks,)),
                dma((FIRST_TILES,)),
                dma((FIRST_CUTS,)),
                dma,
                dma((FIRST_CUTS + CUTS + blocks - 2,)),
                dma,
                dma((blocks - SUBS,)),
                dma,
                dma((blocks - SUBS * 2 + SUBS * LAST_CUTS,)),
                dma,
                dma,
            ],
            compiler_params=pltpu.CompilerParams(
                collective_id=0, has_side_effects=True, vmem_limit_bytes=52 * 2**20
            ),
            cost_estimate=pl.CostEstimate(
                flops=6 * rows * depth * units, bytes_accessed=2 * rows * depth + 6 * depth * units, transcendentals=rows * units
            ),
        )(x, w_gate, w_up, w_down)
        pieces = 8
        return pl.pallas_call(
            functools.partial(write_kernel, pieces),
            out_shape=jax.ShapeDtypeStruct((rows, depth), BF16),
            in_specs=[pl.BlockSpec(memory_space=pltpu.VMEM)],
            out_specs=pl.BlockSpec(memory_space=pltpu.HBM),
            scratch_shapes=[dma((pieces,))],
            compiler_params=pltpu.CompilerParams(has_side_effects=True, vmem_limit_bytes=4 * 2**20),
        )(y)

    return jax.shard_map(
        step,
        mesh=mesh,
        in_specs=(P("dp", None), P(None, "tp"), P(None, "tp"), P("tp", None)),
        out_specs=P("dp", None),
        check_vma=False,
    )
```
